32 devices in a mesh: grp: 16 (over z, y, x), loc: 2 (over core).
Axes of the slice: x: 2, y: 2, z: 4, core: 2. Of those that a mesh axis runs over, the one named last changes fastest.
Arguments:
- tokens: bfloat16 [1024, 3584], P(('grp', 'loc')), may hold values from -6 to 6
- gate_weights: bfloat16 [1024, 8], P(('grp', 'loc')), may hold values from 0.099609375 to 0.59765625
- expert_ids: int32 [1024, 8], P(('grp', 'loc')), may hold values from 0 to 31, as said below
- w_gate: bfloat16 [32, 3584, 1024], P('grp', None, 'loc'), may hold values from -0.09375 to 0.09375
- w_up: bfloat16 [32, 3584, 1024], P('grp', None, 'loc'), may hold values from -0.09375 to 0.09375
- w_down: bfloat16 [32, 3584, 1024], P('grp', None, 'loc'), may hold values from -0.1875 to 0.1875
Outputs:
- layer_out: bfloat16 [1024, 3584], P(('grp', 'loc'))
The draws below stay inside these ranges and needn't reach their ends.
Inputs may be any that keep to these rules, and one draw needn't show every extreme that they name: `expert_ids`: each row names 8 different experts: two in each of 4 different routing groups, a routing group being 4 consecutive expert numbers. Among the rows of one device (aligned blocks of 32 rows) each expert is named at most 16 times, and in every such block some expert is named exactly 16 times.
All inputs are finite; a program needn't handle non-finite values.
Results may differ from the reference program's by a relative error of at most 0.01.
Values may be sent and summed in bfloat16 or wider, within the bound.
A program may use at most 192 MiB of HBM per device.

```python
import jax
import jax.numpy as jnp
from jax import lax

D = 3584
FFE = 1024
RGROUPS = 8
TOPG = 4
TOPK = 8
TOK_DEV = 32
EXPERTS = 32
TOKENS = 1024
MOST = 16
N_LOC = 2


def draw_expert_ids(key, part):
    group_span = EXPERTS // RGROUPS
    block_count = TOKENS // TOK_DEV
    key_first = jax.random.fold_in(key, 11)
    key_second = jax.random.fold_in(key, 12)
    key_rank = jax.random.fold_in(key, 13)
    key_rotation = jax.random.fold_in(key, 14)
    hot_first = jax.random.randint(key_first, (block_count,), 0, RGROUPS)
    hot_second = jax.random.randint(key_second, (block_count,), 0, RGROUPS)
    hot_group = jnp.repeat(jnp.minimum(hot_first, hot_second), TOK_DEV)
    group_index = jnp.arange(RGROUPS, dtype=jnp.int32)
    scores = jax.random.randint(key_rank, (TOKENS, RGROUPS), 0, 1 << 20) * RGROUPS + group_index[None, :]
    scores = jnp.where(group_index[None, :] == hot_group[:, None], 1 << 30, scores)
    chosen = lax.top_k(scores, TOPG)[1].astype(jnp.int32)
    member = jnp.sum((chosen[:, :, None] == group_index[None, None, :]).astype(jnp.int32), axis=1)
    member = member.reshape(block_count, TOK_DEV, RGROUPS)
    order_rank = jnp.cumsum(member, axis=1) - member
    rotation = jax.random.randint(key_rotation, (block_count, 1, RGROUPS), 0, group_span)
    first_local = ((rotation + order_rank) % group_span).reshape(TOKENS, RGROUPS)
    first_pick = jnp.take_along_axis(first_local, chosen, axis=1)
    second_pick = (first_pick + group_span // 2) % group_span
    group_base = chosen * group_span
    expert_pick = jnp.stack([group_base + first_pick, group_base + second_pick], axis=2)
    return expert_pick.reshape(TOKENS, TOPK).astype(jnp.int32)


def shard_levels(rng, extent, pieces, least, high):
    def one(position, parts):
        heights = jax.random.uniform(jax.random.fold_in(jax.random.fold_in(rng, 6), position), (parts,), jnp.float32, least / len(pieces), high / len(pieces))
        return jnp.repeat(jnp.exp(heights), extent[position] // parts).reshape((-1,) + (1,) * (len(extent) - position - 1))

    level = one(*pieces[0])
    for cut in pieces[1:]:
        level = level * one(*cut)
    return level


def centred(own_key, extent, scale, limit, shards=(), kind=jnp.bfloat16):
    values = jax.random.normal(own_key, extent, jnp.float32) * scale
    if len(shards) > 0:
        values = shard_levels(own_key, extent, shards, -0.22, 0.18) * values
    return jnp.clip(values, min=-limit, max=limit).astype(kind)


def setup_inputs(seed: int = 0) -> dict:
    streams_of = jax.random.split(jax.random.key(seed), 7)
    tokens = centred(streams_of[0], (TOKENS, D), 1.0, 6.0, ((0, 32),))
    gate_weights = jnp.clip(0.099609375 + 0.49804688 * jax.random.uniform(streams_of[1], (TOKENS, TOPK), jnp.float32) ** shard_levels(streams_of[1], (TOKENS, TOPK), ((0, 32),), -0.2, 0.2), 0.099609375, 0.59765625).astype(jnp.bfloat16)
    expert_ids = draw_expert_ids(jax.random.fold_in(streams_of[6], 71), 0)
    w_gate = centred(streams_of[3], (EXPERTS, D, FFE), D ** -0.5, 0.09375, ((0, 16), (2, 2)))
    w_up = centred(streams_of[4], (EXPERTS, D, FFE), D ** -0.5, 0.09375, ((0, 16), (2, 2)))
    w_down = centred(streams_of[5], (EXPERTS, D, FFE), FFE ** -0.5, 0.1875, ((0, 16), (2, 2)))
    return dict(tokens=tokens, gate_weights=gate_weights, expert_ids=expert_ids, w_gate=w_gate, w_up=w_up, w_down=w_down)


def reference(tokens, gate_weights, expert_ids, w_gate, w_up, w_down):
    block_count = TOKENS // TOK_DEV
    pair_block = TOK_DEV * TOPK
    per_expert = block_count * MOST
    shard_units = FFE // N_LOC
    block_ids = expert_ids.reshape(block_count, pair_block).astype(jnp.int32)
    same_expert = (block_ids[:, :, None] == block_ids[:, None, :]).astype(jnp.int32)
    pair_order = jnp.arange(pair_block, dtype=jnp.int32)
    earlier = (pair_order[:, None] > pair_order[None, :]).astype(jnp.int32)
    slot_rank = jnp.sum(same_expert * earlier[None], axis=2).astype(jnp.int32)
    block_index = jnp.arange(block_count, dtype=jnp.int32)[:, None]
    target = (block_ids * per_expert + block_index * MOST + slot_rank).reshape(-1).astype(jnp.int32)
    pair_index = jnp.arange(TOKENS * TOPK, dtype=jnp.int32)
    slot_table = jnp.full((EXPERTS * per_expert,), -1, jnp.int32).at[target].set(pair_index)
    slot_table = slot_table.reshape(EXPERTS, per_expert)
    flat_scales = gate_weights.reshape(-1)

    def one_expert(totals, inputs):
        index_row, gate_part, up_part, down_part = inputs
        is_valid = index_row >= 0
        safe_index = jnp.maximum(index_row, 0).astype(jnp.int32)
        token_row = (safe_index // TOPK).astype(jnp.int32)
        rows_in = tokens[token_row]
        scales = jnp.where(is_valid, flat_scales[safe_index].astype(jnp.float32), jnp.zeros((), jnp.float32))
        gate_act = jnp.dot(rows_in, gate_part, preferred_element_type=jnp.float32)
        upward = jnp.dot(rows_in, up_part, preferred_element_type=jnp.float32)
        hidden = (jax.nn.silu(gate_act) * upward).astype(jnp.bfloat16)
        blocked = hidden.reshape(per_expert, N_LOC, shard_units).astype(jnp.float32)
        down_blocks = down_part.reshape(D, N_LOC, shard_units).astype(jnp.float32)
        partial_value = jnp.einsum("rlf,dlf->rld", blocked, down_blocks)
        partial_value = lax.optimization_barrier((partial_value * scales[:, None, None]).astype(jnp.bfloat16))
        outcome = jnp.sum(partial_value.astype(jnp.float32), axis=1).astype(jnp.bfloat16)
        outcome = lax.optimization_barrier(outcome)
        return totals.at[token_row].add(outcome.astype(jnp.float32)), None

    start_totals = jnp.zeros((TOKENS, D), jnp.float32)
    totals = lax.scan(one_expert, start_totals, (slot_table, w_gate, w_up, w_down))[0]
    return totals.astype(jnp.bfloat16)
```

```python
import functools

import jax
import jax.numpy as jnp
from jax import lax
from jax.experimental import pallas as pl
from jax.experimental.pallas import tpu as pltpu
from jax.sharding import PartitionSpec as P

RGROUPS = 8
LANES = 128
MESH = pl.DeviceIdType.MESH


class Place:
    def __init__(self, columns):
        self.deep = columns // 4
        self.g = lax.axis_index("grp")
        self.c = lax.axis_index("loc")
        self.x = lax.rem(self.g, 2)
        self.y = lax.rem(lax.div(self.g, 2), 2)
        self.z = lax.div(self.g, 4)
        self.below = self.z > 0
        self.above = self.z < self.deep - 1

    def at(self, dz=0, fx=0, fy=0):
        x = 1 - self.x if fx else self.x
        y = 1 - self.y if fy else self.y
        return (self.z + dz) * 4 + y * 2 + x

    def line(self, step):
        if step == 0:
            return [(0, None)]
        return [(-step, self.z >= step), (step, self.z + step < self.deep)]


def when(cond, act):
    if cond is None:
        act()
    else:
        pl.when(cond)(act)


def greet(me):
    barrier = pltpu.get_barrier_semaphore()
    partners = [
        (None, me.at(fx=1), me.c),
        (None, me.at(fy=1), me.c),
        (None, me.g, 1 - me.c),
        (me.below, me.at(dz=-1), me.c),
        (me.above, me.at(dz=1), me.c),
    ]
    for cond, g, c in partners:
        when(cond, lambda g=g, c=c: pl.semaphore_signal(
            barrier, inc=1, device_id=(g, c), device_id_type=MESH))
    edges = (me.z > 0).astype(jnp.int32) + (me.z < me.deep - 1).astype(jnp.int32)
    pl.semaphore_wait(barrier, 3 + edges)


def gather_kernel(columns, own_ref, out_ref, own_sem, send_sem, ici_sem, loc_sem):
    me = Place(columns)
    rows = own_ref.shape[0]
    half = rows // 2
    greet(me)

    def slot(h, g, c):
        return out_ref.at[pl.ds(pl.multiple_of((g * 2 + c) * rows + h * half, half), half)]

    base = pl.multiple_of((me.g * 2 + me.c) * rows, rows)
    keep = pltpu.make_async_copy(own_ref, out_ref.at[pl.ds(base, rows)], own_sem)
    keep.start()
    sends = []

    def push(cond, h, g, kind, device, own):
        source = own_ref.at[pl.ds(h * half, half)] if own else slot(h, g, me.c)
        arrive = loc_sem if kind == 4 else ici_sem
        copy = pltpu.make_async_remote_copy(
            src_ref=source, dst_ref=slot(h, g, me.c),
            send_sem=send_sem.at[h, g, kind], recv_sem=arrive.at[h, g],
            device_id=device, device_id_type=MESH)
        when(cond, copy.start)
        sends.append((cond, copy))

    def arrived(cond, h, g):
        copy = pltpu.make_async_remote_copy(
            src_ref=slot(h, g, me.c), dst_ref=slot(h, g, me.c),
            send_sem=send_sem.at[h, g, 0], recv_sem=ici_sem.at[h, g],
            device_id=(me.g, 1 - me.c), device_id_type=MESH)
        when(cond, copy.wait_recv)

    def both(a, b):
        return b if a is None else jnp.logical_and(a, b)

    flips = [dict(fx=1), dict(fy=1)]

    def first(step):
        for dz, cond in me.line(step):
            for h in range(2):
                g = me.at(dz)
                if step:
                    arrived(cond, h, g)
                if dz <= 0:
                    push(both(cond, me.above), h, g, 0, (me.at(1), me.c), step == 0)
                if dz >= 0:
                    push(both(cond, me.below), h, g, 1, (me.at(-1), me.c), step == 0)
                push(cond, h, g, 2, (me.at(**flips[h]), me.c), step == 0)
                push(cond, h, g, 3, (me.at(**flips[1 - h]), me.c), step == 0)
                push(cond, h, g, 4, (me.g, 1 - me.c), step == 0)

    def second(step):
        for dz, cond in me.line(step):
            for h in range(2):
                g = me.at(dz, **flips[h])
                arrived(cond, h, g)
                push(cond, h, g, 3, (me.at(**flips[1 - h]), me.c), False)
                push(cond, h, g, 4, (me.g, 1 - me.c), False)

    def third(step):
        for dz, cond in me.line(step):
            for h in range(2):
                for g in (me.at(dz, **flips[1 - h]), me.at(dz, fx=1, fy=1)):
                    arrived(cond, h, g)
                    push(cond, h, g, 4, (me.g, 1 - me.c), False)

    for turn in range(me.deep + 2):
        for stage, lag in ((first, 0), (second, 1), (third, 2)):
            if 0 <= turn - lag < me.deep:
                stage(turn - lag)
    for h in range(2):
        for g in range(columns):
            pltpu.make_async_remote_copy(
                src_ref=slot(h, g, 1 - me.c), dst_ref=slot(h, g, 1 - me.c),
                send_sem=send_sem.at[h, g, 4], recv_sem=loc_sem.at[h, g],
                device_id=(me.g, 1 - me.c), device_id_type=MESH).wait_recv()
    for cond, copy in sends:
        when(cond, copy.wait_send)
    keep.wait()


def gather_tokens(joined, columns):
    rows, width = joined.shape
    dma = pltpu.SemaphoreType.DMA
    return pl.pallas_call(
        functools.partial(gather_kernel, columns),
        out_shape=jax.ShapeDtypeStruct((columns * 2 * rows, width), joined.dtype),
        in_specs=[pl.BlockSpec(memory_space=pltpu.VMEM)],
        out_specs=pl.BlockSpec(memory_space=pltpu.VMEM),
        scratch_shapes=[dma, dma((2, columns, 5)), dma((2, columns)), dma((2, columns))],
        compiler_params=pltpu.CompilerParams(
            collective_id=1, has_side_effects=True, vmem_limit_bytes=24 * 2**20),
        name="gather_tokens",
    )(joined)


def scatter_kernel(columns, part_ref, out_ref, sums, from_loc, from_two, from_one, from_low,
                   from_high, loc_send, send_sem, loc_sem, two_sem, one_sem, low_sem, high_sem):
    me = Place(columns)
    rows = out_ref.shape[0]
    half = rows // 2
    width = out_ref.shape[1]
    piece = width // 4 if width % (4 * LANES) == 0 else width
    greet(me)
    flips = [dict(fx=1), dict(fy=1)]
    sends = []

    def start(h, g):
        return pl.multiple_of((g * 2 + me.c) * rows + h * half, half)

    def to_core(h, g, cond):
        base = pl.multiple_of((g * 2 + 1 - me.c) * rows + h * half, half)
        copy = pltpu.make_async_remote_copy(
            src_ref=part_ref.at[pl.ds(base, half)], dst_ref=from_loc.at[h, g],
            send_sem=loc_send.at[h, g], recv_sem=loc_sem.at[h, g],
            device_id=(me.g, 1 - me.c), device_id_type=MESH)
        when(cond, copy.start)
        sends.append((cond, copy))

    def send(cond, h, g, buffer, sem, device):
        copy = pltpu.make_async_remote_copy(
            src_ref=sums.at[h, g], dst_ref=buffer.at[h, g],
            send_sem=send_sem.at[h, g], recv_sem=sem.at[h, g],
            device_id=device, device_id_type=MESH)
        when(cond, copy.start)
        sends.append((cond, copy))

    def add(h, g, terms, final=False):
        for buffer, sem in terms:
            pltpu.make_async_remote_copy(
                src_ref=buffer.at[h, g], dst_ref=buffer.at[h, g],
                send_sem=send_sem.at[h, g], recv_sem=sem.at[h, g],
                device_id=(me.g, 1 - me.c), device_id_type=MESH).wait_recv()
        for low in range(0, width, piece):
            cols = slice(low, low + piece)
            total = part_ref[pl.ds(start(h, g), half), cols].astype(jnp.float32)
            for buffer, _ in terms:
                total = total + buffer[h, g, :, cols].astype(jnp.float32)
            if final:
                out_ref[h * half:(h + 1) * half, cols] = total.astype(out_ref.dtype)
            else:
                sums[h, g, :, cols] = total.astype(sums.dtype)

    loc, two, one = (from_loc, loc_sem), (from_two, two_sem), (from_one, one_sem)
    low, high = (from_low, low_sem), (from_high, high_sem)

    def third(step, act):
        for h in range(2):
            for dz, cond in me.line(step):
                for g in (me.at(dz, fx=1, fy=1), me.at(dz, **flips[1 - h])):
                    act(h, g, cond)

    def second(step, act):
        for h in range(2):
            for dz, cond in me.line(step):
                act(h, me.at(dz, **flips[h]), cond)

    def first(step, act):
        for h in range(2):
            for dz, cond in me.line(step):
                act(h, me.at(dz), cond, dz)

    steps = range(me.deep - 1, -1, -1)
    for step in steps:
        third(step, to_core)
    for step in steps:
        second(step, to_core)
        first(step, lambda h, g, cond, dz: to_core(h, g, cond))

    def cross_two(h, g, cond):
        when(cond, lambda: add(h, g, [loc]))
        send(cond, h, g, from_two, two_sem, (me.at(**flips[1 - h]), me.c))

    def cross_one(h, g, cond):
        when(cond, lambda: add(h, g, [loc, two]))
        send(cond, h, g, from_one, one_sem, (me.at(**flips[h]), me.c))

    def cross_line(h, g, cond, dz):
        if dz > 0:
            edge, near, away = me.below, low, me.at(1)
        elif dz < 0:
            edge, near, away = me.above, high, me.at(-1)
        else:
            for under in (False, True):
                for over in (False, True):
                    if me.deep == 1 and (under or over):
                        continue
                    fits = jnp.logical_and(me.below == under, me.above == over)
                    terms = [loc, two, one] + [low] * under + [high] * over
                    pl.when(fits)(lambda terms=terms: add(h, g, terms, True))
            return
        pl.when(jnp.logical_and(cond, edge))(lambda: add(h, g, [loc, two, one, near]))
        inner = jnp.logical_and(cond, jnp.logical_not(edge))
        pl.when(inner)(lambda: add(h, g, [loc, two, one]))
        target = low if dz > 0 else high
        send(cond, h, g, target[0], target[1], (away, me.c))

    for turn in range(me.deep + 2):
        for stage, act, lag in ((third, cross_two, 0), (second, cross_one, 1), (first, cross_line, 2)):
            if 0 <= turn - lag < me.deep:
                stage(me.deep - 1 - (turn - lag), act)
    for cond, copy in sends:
        when(cond, copy.wait_send)


def scatter_sums(partial, columns):
    rows = partial.shape[0] // (2 * columns)
    width = partial.shape[1]
    dma = pltpu.SemaphoreType.DMA
    buffer = pltpu.VMEM((2, columns, rows // 2, width), partial.dtype)
    return pl.pallas_call(
        functools.partial(scatter_kernel, columns),
        out_shape=jax.ShapeDtypeStruct((rows, width), partial.dtype),
        in_specs=[pl.BlockSpec(memory_space=pltpu.VMEM)],
        out_specs=pl.BlockSpec(memory_space=pltpu.VMEM),
        scratch_shapes=[buffer] * 6 + [dma((2, columns))] * 7,
        compiler_params=pltpu.CompilerParams(
            collective_id=2, has_side_effects=True, vmem_limit_bytes=48 * 2**20),
        name="scatter_sums",
    )(partial)


def dense_body(tokens, gate_weights, expert_ids, w_gate, w_up, w_down):
    width = tokens.shape[1]
    local_experts = w_gate.shape[0]
    columns = lax.axis_size("grp")
    expert_total = columns * local_experts
    padded = -(-expert_total // LANES) * LANES
    numbers = jnp.arange(padded, dtype=jnp.int32)
    chosen = expert_ids[:, :, None] == numbers[None, None, :]
    table = jnp.sum(
        jnp.where(chosen, gate_weights.astype(jnp.float32)[:, :, None], 0.0), axis=1
    ).astype(jnp.bfloat16)
    gathered = gather_tokens(jnp.concatenate([tokens, table], axis=1), columns)
    rows = gathered[:, :width]
    first = width + lax.axis_index("grp") * local_experts
    scales = lax.dynamic_slice_in_dim(gathered, first, local_experts, axis=1).astype(jnp.float32)
    hidden = []
    for expert in range(local_experts):
        gate_act = jnp.dot(rows, w_gate[expert], preferred_element_type=jnp.float32)
        upward = jnp.dot(rows, w_up[expert], preferred_element_type=jnp.float32)
        value = jax.nn.silu(gate_act) * upward * scales[:, expert : expert + 1]
        hidden.append(value.astype(jnp.bfloat16))
    partial = None
    for expert in range(local_experts):
        term = lax.dot_general(
            hidden[expert], w_down[expert], (((1,), (1,)), ((), ())),
            preferred_element_type=jnp.float32,
        )
        partial = term if partial is None else partial + term
    return scatter_sums(partial.astype(jnp.bfloat16), columns)


def expert_rows(inputs, scales, gate_part, up_part, down_part):
    gate_act = jnp.dot(inputs, gate_part, preferred_element_type=jnp.float32)
    upward = jnp.dot(inputs, up_part, preferred_element_type=jnp.float32)
    hidden = (jax.nn.silu(gate_act) * upward).astype(jnp.bfloat16)
    projected = lax.dot_general(
        hidden, down_part, (((1,), (1,)), ((), ())), preferred_element_type=jnp.float32
    )
    return projected * scales.astype(jnp.float32)[:, None]


def weights_path(rows_in, scales_in, w_gate, w_up, w_down):
    row_dims = rows_in.shape
    shard_units = w_gate.shape[2]
    expert_inputs = [rows_in[:, expert].reshape(-1, row_dims[3]) for expert in range(row_dims[1])]
    expert_scales = [scales_in[:, expert].reshape(-1) for expert in range(row_dims[1])]
    starting = tuple(
        (
            jnp.zeros((row_dims[0] * row_dims[2], row_dims[3]), jnp.float32)
            for expert in range(row_dims[1])
        )
    )
    gate_piece = lax.all_gather(w_gate, "loc", axis=2, tiled=True)
    up_piece = lax.all_gather(w_up, "loc", axis=2, tiled=True)
    down_piece = lax.all_gather(w_down, "loc", axis=2, tiled=True)
    updated = []
    for expert in range(row_dims[1]):
        running = starting[expert]
        for block_index in range(gate_piece.shape[2] // shard_units):
            lower_unit = block_index * shard_units
            upper_unit = lower_unit + shard_units
            values = expert_rows(
                expert_inputs[expert],
                expert_scales[expert],
                gate_piece[expert][:, lower_unit:upper_unit],
                up_piece[expert][:, lower_unit:upper_unit],
                down_piece[expert][:, lower_unit:upper_unit],
            )
            rounded = lax.optimization_barrier(values.astype(jnp.bfloat16))
            running = running + rounded.astype(jnp.float32)
        updated.append(running)
    folded = tuple(updated)
    stacked = jnp.stack(
        [folded_part.reshape(row_dims[0], row_dims[2], row_dims[3]) for folded_part in folded],
        axis=1,
    )
    return stacked.astype(jnp.bfloat16)


def slot_body(tokens, gate_weights, expert_ids, w_gate, w_up, w_down):
    tok_count = tokens.shape[0]
    choices_per = expert_ids.shape[1]
    feature_count = tokens.shape[1]
    group_count = lax.axis_size("grp")
    local_experts = w_gate.shape[0]
    expert_total = group_count * local_experts
    slot_depth = 2 * tok_count * RGROUPS // expert_total
    slot_total = expert_total * slot_depth
    pair_ids = expert_ids.reshape(-1)
    pair_count = pair_ids.shape[0]
    pair_order = jnp.arange(pair_count, dtype=jnp.int32)
    same_expert = (pair_ids[:, None] == pair_ids[None, :]).astype(jnp.int32)
    earlier = (pair_order[:, None] > pair_order[None, :]).astype(jnp.int32)
    slot_rank = jnp.sum(same_expert * earlier, axis=1)
    position = pair_ids * slot_depth + slot_rank
    pair_onehot = jnp.arange(slot_total, dtype=jnp.int32)[:, None] == position[None, :]
    placement = jnp.sum(
        pair_onehot.reshape(slot_total, tok_count, choices_per).astype(jnp.int32), axis=2
    ).astype(jnp.bfloat16)
    send_rows = jnp.dot(placement, tokens, preferred_element_type=jnp.float32).astype(jnp.bfloat16)
    flat_scales = gate_weights.reshape(-1).astype(jnp.float32)
    send_scales = jnp.sum(jnp.where(pair_onehot, flat_scales[None, :], 0.0), axis=1).astype(
        jnp.bfloat16
    )
    send_rows = send_rows.reshape(group_count, local_experts, slot_depth, feature_count)
    send_scales = send_scales.reshape(group_count, local_experts, slot_depth)
    computed = weights_path(
        lax.all_to_all(send_rows, "grp", split_axis=0, concat_axis=0, tiled=True),
        lax.all_to_all(send_scales, "grp", split_axis=0, concat_axis=0, tiled=True),
        w_gate,
        w_up,
        w_down,
    )
    returned = lax.all_to_all(computed, "grp", split_axis=0, concat_axis=0, tiled=True)
    flat_back = returned.reshape(slot_total, feature_count)
    mixed_out = lax.dot_general(
        placement, flat_back, (((0,), (0,)), ((), ())), preferred_element_type=jnp.float32
    )
    return mixed_out.astype(jnp.bfloat16)


def body(tokens, gate_weights, expert_ids, w_gate, w_up, w_down):
    tok_count = tokens.shape[0]
    columns = lax.axis_size("grp")
    slot_depth = 2 * tok_count * RGROUPS // (columns * w_gate.shape[0])
    dense = slot_depth * w_gate.shape[0] >= tok_count
    fits = columns % 4 == 0 and lax.axis_size("loc") == 2 and tok_count % 32 == 0
    chosen = dense_body if dense and fits else slot_body
    return chosen(tokens, gate_weights, expert_ids, w_gate, w_up, w_down)


def solution(mesh):
    placed = (
        P(("grp", "loc"), None),
        P(("grp", "loc"), None),
        P(("grp", "loc"), None),
        P("grp", None, "loc"),
        P("grp", None, "loc"),
        P("grp", None, "loc"),
    )
    return jax.shard_map(
        body, mesh=mesh, in_specs=placed, out_specs=P(("grp", "loc"), None), check_vma=False
    )
```

```python
import functools

import jax
import jax.numpy as jnp
from jax import lax
from jax.experimental import pallas as pl
from jax.experimental.pallas import tpu as pltpu
from jax.sharding import PartitionSpec as P

RGROUPS = 8
LANES = 128
MESH = pl.DeviceIdType.MESH


class Place:
    def __init__(self, columns):
        self.deep = columns // 4
        self.g = lax.axis_index("grp")
        self.c = lax.axis_index("loc")
        self.x = lax.rem(self.g, 2)
        self.y = lax.rem(lax.div(self.g, 2), 2)
        self.z = lax.div(self.g, 4)
        self.below = self.z > 0
        self.above = self.z < self.deep - 1

    def at(self, dz=0, fx=0, fy=0):
        x = 1 - self.x if fx else self.x
        y = 1 - self.y if fy else self.y
        return (self.z + dz) * 4 + y * 2 + x

    def line(self, step):
        if step == 0:
            return [(0, None)]
        return [(-step, self.z >= step), (step, self.z + step < self.deep)]


def when(cond, act):
    if cond is None:
        act()
    else:
        pl.when(cond)(act)


def greet(me):
    barrier = pltpu.get_barrier_semaphore()
    partners = [
        (None, me.at(fx=1), me.c),
        (None, me.at(fy=1), me.c),
        (None, me.g, 1 - me.c),
        (me.below, me.at(dz=-1), me.c),
        (me.above, me.at(dz=1), me.c),
    ]
    for cond, g, c in partners:
        when(cond, lambda g=g, c=c: pl.semaphore_signal(
            barrier, inc=1, device_id=(g, c), device_id_type=MESH))
    edges = (me.z > 0).astype(jnp.int32) + (me.z < me.deep - 1).astype(jnp.int32)
    pl.semaphore_wait(barrier, 3 + edges)


def gather_kernel(columns, own_ref, out_ref, own_sem, send_sem, ici_sem, loc_sem):
    me = Place(columns)
    rows = own_ref.shape[0]
    half = rows // 2
    greet(me)

    def slot(h, g, c):
        return out_ref.at[pl.ds(pl.multiple_of((g * 2 + c) * rows + h * half, half), half)]

    base = pl.multiple_of((me.g * 2 + me.c) * rows, rows)
    keep = pltpu.make_async_copy(own_ref, out_ref.at[pl.ds(base, rows)], own_sem)
    keep.start()
    sends = []

    def push(cond, h, g, kind, device, own):
        source = own_ref.at[pl.ds(h * half, half)] if own else slot(h, g, me.c)
        arrive = loc_sem if kind == 4 else ici_sem
        copy = pltpu.make_async_remote_copy(
            src_ref=source, dst_ref=slot(h, g, me.c),
            send_sem=send_sem.at[h, g, kind], recv_sem=arrive.at[h, g],
            device_id=device, device_id_type=MESH)
        when(cond, copy.start)
        sends.append((cond, copy))

    def arrived(cond, h, g):
        copy = pltpu.make_async_remote_copy(
            src_ref=slot(h, g, me.c), dst_ref=slot(h, g, me.c),
            send_sem=send_sem.at[h, g, 0], recv_sem=ici_sem.at[h, g],
            device_id=(me.g, 1 - me.c), device_id_type=MESH)
        when(cond, copy.wait_recv)

    def both(a, b):
        return b if a is None else jnp.logical_and(a, b)

    flips = [dict(fx=1), dict(fy=1)]

    def first(step):
        for dz, cond in me.line(step):
            for h in range(2):
                g = me.at(dz)
                if step:
                    arrived(cond, h, g)
                if dz <= 0:
                    push(both(cond, me.above), h, g, 0, (me.at(1), me.c), step == 0)
                if dz >= 0:
                    push(both(cond, me.below), h, g, 1, (me.at(-1), me.c), step == 0)
                push(cond, h, g, 2, (me.at(**flips[h]), me.c), step == 0)
                push(cond, h, g, 3, (me.at(**flips[1 - h]), me.c), step == 0)
                push(cond, h, g, 4, (me.g, 1 - me.c), step == 0)

    def second(step):
        for dz, cond in me.line(step):
            for h in range(2):
                g = me.at(dz, **flips[h])
                arrived(cond, h, g)
                push(cond, h, g, 3, (me.at(**flips[1 - h]), me.c), False)
                push(cond, h, g, 4, (me.g, 1 - me.c), False)

    def third(step):
        for dz, cond in me.line(step):
            for h in range(2):
                for g in (me.at(dz, **flips[1 - h]), me.at(dz, fx=1, fy=1)):
                    arrived(cond, h, g)
                    push(cond, h, g, 4, (me.g, 1 - me.c), False)

    for turn in range(me.deep + 2):
        for stage, lag in ((first, 0), (second, 1), (third, 2)):
            if 0 <= turn - lag < me.deep:
                stage(turn - lag)
    for h in range(2):
        for g in range(columns):
            pltpu.make_async_remote_copy(
                src_ref=slot(h, g, 1 - me.c), dst_ref=slot(h, g, 1 - me.c),
                send_sem=send_sem.at[h, g, 4], recv_sem=loc_sem.at[h, g],
                device_id=(me.g, 1 - me.c), device_id_type=MESH).wait_recv()
    for cond, copy in sends:
        when(cond, copy.wait_send)
    keep.wait()


def gather_tokens(joined, columns):
    rows, width = joined.shape
    dma = pltpu.SemaphoreType.DMA
    return pl.pallas_call(
        functools.partial(gather_kernel, columns),
        out_shape=jax.ShapeDtypeStruct((columns * 2 * rows, width), joined.dtype),
        in_specs=[pl.BlockSpec(memory_space=pltpu.VMEM)],
        out_specs=pl.BlockSpec(memory_space=pltpu.VMEM),
        scratch_shapes=[dma, dma((2, columns, 5)), dma((2, columns)), dma((2, columns))],
        compiler_params=pltpu.CompilerParams(
            collective_id=1, has_side_effects=True, vmem_limit_bytes=24 * 2**20),
        name="gather_tokens",
    )(joined)


def scatter_kernel(columns, part_ref, out_ref, sums, from_loc, from_two, from_one, from_low,
                   from_high, loc_send, send_sem, loc_sem, two_sem, one_sem, low_sem, high_sem):
    me = Place(columns)
    rows = out_ref.shape[0]
    half = rows // 2
    width = out_ref.shape[1]
    piece = width // 4 if width % (4 * LANES) == 0 else width
    greet(me)
    flips = [dict(fx=1), dict(fy=1)]
    sends = []

    def start(h, g):
        return pl.multiple_of((g * 2 + me.c) * rows + h * half, half)

    def to_core(h, g, cond):
        base = pl.multiple_of((g * 2 + 1 - me.c) * rows + h * half, half)
        copy = pltpu.make_async_remote_copy(
            src_ref=part_ref.at[pl.ds(base, half)], dst_ref=from_loc.at[h, g],
            send_sem=loc_send.at[h, g], recv_sem=loc_sem.at[h, g],
            device_id=(me.g, 1 - me.c), device_id_type=MESH)
        when(cond, copy.start)
        sends.append((cond, copy))

    def send(cond, h, g, buffer, sem, device):
        copy = pltpu.make_async_remote_copy(
            src_ref=sums.at[h, g], dst_ref=buffer.at[h, g],
            send_sem=send_sem.at[h, g], recv_sem=sem.at[h, g],
            device_id=device, device_id_type=MESH)
        when(cond, copy.start)
        sends.append((cond, copy))

    def add(h, g, terms, final=False):
        for buffer, sem in terms:
            pltpu.make_async_remote_copy(
                src_ref=buffer.at[h, g], dst_ref=buffer.at[h, g],
                send_sem=send_sem.at[h, g], recv_sem=sem.at[h, g],
                device_id=(me.g, 1 - me.c), device_id_type=MESH).wait_recv()
        for low in range(0, width, piece):
            cols = slice(low, low + piece)
            total = part_ref[pl.ds(start(h, g), half), cols].astype(jnp.float32)
            for buffer, _ in terms:
                total = total + buffer[h, g, :, cols].astype(jnp.float32)
            if final:
                out_ref[h * half:(h + 1) * half, cols] = total.astype(out_ref.dtype)
            else:
                sums[h, g, :, cols] = total.astype(sums.dtype)

    loc, two, one = (from_loc, loc_sem), (from_two, two_sem), (from_one, one_sem)
    low, high = (from_low, low_sem), (from_high, high_sem)

    def third(step, act):
        for h in range(2):
            for dz, cond in me.line(step):
                for g in (me.at(dz, fx=1, fy=1), me.at(dz, **flips[1 - h])):
                    act(h, g, cond)

    def second(step, act):
        for h in range(2):
            for dz, cond in me.line(step):
                act(h, me.at(dz, **flips[h]), cond)

    def first(step, act):
        for h in range(2):
            for dz, cond in me.line(step):
                act(h, me.at(dz), cond, dz)

    steps = range(me.deep - 1, -1, -1)
    for step in steps:
        third(step, to_core)
    for step in steps:
        second(step, to_core)
        first(step, lambda h, g, cond, dz: to_core(h, g, cond))

    def cross_two(h, g, cond):
        when(cond, lambda: add(h, g, [loc]))
        send(cond, h, g, from_two, two_sem, (me.at(**flips[1 - h]), me.c))

    def cross_one(h, g, cond):
        when(cond, lambda: add(h, g, [loc, two]))
        send(cond, h, g, from_one, one_sem, (me.at(**flips[h]), me.c))

    def cross_line(h, g, cond, dz):
        if dz > 0:
            edge, near, away = me.below, low, me.at(1)
        elif dz < 0:
            edge, near, away = me.above, high, me.at(-1)
        else:
            for under in (False, True):
                for over in (False, True):
                    if me.deep == 1 and (under or over):
                        continue
                    fits = jnp.logical_and(me.below == under, me.above == over)
                    terms = [loc, two, one] + [low] * under + [high] * over
                    pl.when(fits)(lambda terms=terms: add(h, g, terms, True))
            return
        pl.when(jnp.logical_and(cond, edge))(lambda: add(h, g, [loc, two, one, near]))
        inner = jnp.logical_and(cond, jnp.logical_not(edge))
        pl.when(inner)(lambda: add(h, g, [loc, two, one]))
        target = low if dz > 0 else high
        send(cond, h, g, target[0], target[1], (away, me.c))

    for turn in range(me.deep + 2):
        for stage, act, lag in ((third, cross_two, 0), (second, cross_one, 1), (first, cross_line, 2)):
            if 0 <= turn - lag < me.deep:
                stage(me.deep - 1 - (turn - lag), act)
    for cond, copy in sends:
        when(cond, copy.wait_send)


def scatter_sums(partial, columns):
    rows = partial.shape[0] // (2 * columns)
    width = partial.shape[1]
    dma = pltpu.SemaphoreType.DMA
    buffer = pltpu.VMEM((2, columns, rows // 2, width), partial.dtype)
    return pl.pallas_call(
        functools.partial(scatter_kernel, columns),
        out_shape=jax.ShapeDtypeStruct((rows, width), partial.dtype),
        in_specs=[pl.BlockSpec(memory_space=pltpu.VMEM)],
        out_specs=pl.BlockSpec(memory_space=pltpu.VMEM),
        scratch_shapes=[buffer] * 6 + [dma((2, columns))] * 7,
        compiler_params=pltpu.CompilerParams(
            collective_id=2, has_side_effects=True, vmem_limit_bytes=34 * 2**20),
        name="scatter_sums",
    )(partial)


def down_kernel(*refs):
    *hidden, down_ref, out_ref = refs
    total = None
    for expert, ref in enumerate(hidden):
        term = lax.dot_general(
            ref[...], down_ref[expert], (((1,), (1,)), ((), ())),
            preferred_element_type=jnp.float32)
        total = term if total is None else total + term
    out_ref[...] = total.astype(out_ref.dtype)


def project_down(hidden, w_down):
    experts, width, units = w_down.shape
    rows = hidden[0].shape[0]
    tile = 512 if width % 512 == 0 else width
    return pl.pallas_call(
        down_kernel,
        grid=(width // tile,),
        out_shape=jax.ShapeDtypeStruct((rows, width), jnp.bfloat16),
        in_specs=[pl.BlockSpec((rows, units), lambda i: (0, 0))] * experts
        + [pl.BlockSpec((experts, tile, units), lambda i: (0, i, 0))],
        out_specs=pl.BlockSpec((rows, tile), lambda i: (0, i)),
        compiler_params=pltpu.CompilerParams(vmem_limit_bytes=24 * 2**20),
        name="project_down",
    )(*hidden, w_down)


def dense_body(tokens, gate_weights, expert_ids, w_gate, w_up, w_down):
    width = tokens.shape[1]
    local_experts = w_gate.shape[0]
    columns = lax.axis_size("grp")
    expert_total = columns * local_experts
    padded = -(-expert_total // LANES) * LANES
    numbers = jnp.arange(padded, dtype=jnp.int32)
    chosen = expert_ids[:, :, None] == numbers[None, None, :]
    table = jnp.sum(
        jnp.where(chosen, gate_weights.astype(jnp.float32)[:, :, None], 0.0), axis=1
    ).astype(jnp.bfloat16)
    gathered = gather_tokens(jnp.concatenate([tokens, table], axis=1), columns)
    rows = gathered[:, :width]
    first = width + lax.axis_index("grp") * local_experts
    scales = lax.dynamic_slice_in_dim(gathered, first, local_experts, axis=1).astype(jnp.float32)
    hidden = []
    for expert in range(local_experts):
        gate_act = lax.optimization_barrier(
            jnp.dot(rows, w_gate[expert], preferred_element_type=jnp.float32))
        upward = jnp.dot(rows, w_up[expert], preferred_element_type=jnp.float32)
        value = jax.nn.silu(gate_act) * upward * scales[:, expert : expert + 1]
        hidden.append(value.astype(jnp.bfloat16))
    partial = project_down(lax.optimization_barrier(tuple(hidden)), w_down)
    return scatter_sums(partial, columns)


def expert_rows(inputs, scales, gate_part, up_part, down_part):
    gate_act = jnp.dot(inputs, gate_part, preferred_element_type=jnp.float32)
    upward = jnp.dot(inputs, up_part, preferred_element_type=jnp.float32)
    hidden = (jax.nn.silu(gate_act) * upward).astype(jnp.bfloat16)
    projected = lax.dot_general(
        hidden, down_part, (((1,), (1,)), ((), ())), preferred_element_type=jnp.float32
    )
    return projected * scales.astype(jnp.float32)[:, None]


def weights_path(rows_in, scales_in, w_gate, w_up, w_down):
    row_dims = rows_in.shape
    shard_units = w_gate.shape[2]
    expert_inputs = [rows_in[:, expert].reshape(-1, row_dims[3]) for expert in range(row_dims[1])]
    expert_scales = [scales_in[:, expert].reshape(-1) for expert in range(row_dims[1])]
    starting = tuple(
        (
            jnp.zeros((row_dims[0] * row_dims[2], row_dims[3]), jnp.float32)
            for expert in range(row_dims[1])
        )
    )
    gate_piece = lax.all_gather(w_gate, "loc", axis=2, tiled=True)
    up_piece = lax.all_gather(w_up, "loc", axis=2, tiled=True)
    down_piece = lax.all_gather(w_down, "loc", axis=2, tiled=True)
    updated = []
    for expert in range(row_dims[1]):
        running = starting[expert]
        for block_index in range(gate_piece.shape[2] // shard_units):
            lower_unit = block_index * shard_units
            upper_unit = lower_unit + shard_units
            values = expert_rows(
                expert_inputs[expert],
                expert_scales[expert],
                gate_piece[expert][:, lower_unit:upper_unit],
                up_piece[expert][:, lower_unit:upper_unit],
                down_piece[expert][:, lower_unit:upper_unit],
            )
            rounded = lax.optimization_barrier(values.astype(jnp.bfloat16))
            running = running + rounded.astype(jnp.float32)
        updated.append(running)
    folded = tuple(updated)
    stacked = jnp.stack(
        [folded_part.reshape(row_dims[0], row_dims[2], row_dims[3]) for folded_part in folded],
        axis=1,
    )
    return stacked.astype(jnp.bfloat16)


def slot_body(tokens, gate_weights, expert_ids, w_gate, w_up, w_down):
    tok_count = tokens.shape[0]
    choices_per = expert_ids.shape[1]
    feature_count = tokens.shape[1]
    group_count = lax.axis_size("grp")
    local_experts = w_gate.shape[0]
    expert_total = group_count * local_experts
    slot_depth = 2 * tok_count * RGROUPS // expert_total
    slot_total = expert_total * slot_depth
    pair_ids = expert_ids.reshape(-1)
    pair_count = pair_ids.shape[0]
    pair_order = jnp.arange(pair_count, dtype=jnp.int32)
    same_expert = (pair_ids[:, None] == pair_ids[None, :]).astype(jnp.int32)
    earlier = (pair_order[:, None] > pair_order[None, :]).astype(jnp.int32)
    slot_rank = jnp.sum(same_expert * earlier, axis=1)
    position = pair_ids * slot_depth + slot_rank
    pair_onehot = jnp.arange(slot_total, dtype=jnp.int32)[:, None] == position[None, :]
    placement = jnp.sum(
        pair_onehot.reshape(slot_total, tok_count, choices_per).astype(jnp.int32), axis=2
    ).astype(jnp.bfloat16)
    send_rows = jnp.dot(placement, tokens, preferred_element_type=jnp.float32).astype(jnp.bfloat16)
    flat_scales = gate_weights.reshape(-1).astype(jnp.float32)
    send_scales = jnp.sum(jnp.where(pair_onehot, flat_scales[None, :], 0.0), axis=1).astype(
        jnp.bfloat16
    )
    send_rows = send_rows.reshape(group_count, local_experts, slot_depth, feature_count)
    send_scales = send_scales.reshape(group_count, local_experts, slot_depth)
    computed = weights_path(
        lax.all_to_all(send_rows, "grp", split_axis=0, concat_axis=0, tiled=True),
        lax.all_to_all(send_scales, "grp", split_axis=0, concat_axis=0, tiled=True),
        w_gate,
        w_up,
        w_down,
    )
    returned = lax.all_to_all(computed, "grp", split_axis=0, concat_axis=0, tiled=True)
    flat_back = returned.reshape(slot_total, feature_count)
    mixed_out = lax.dot_general(
        placement, flat_back, (((0,), (0,)), ((), ())), preferred_element_type=jnp.float32
    )
    return mixed_out.astype(jnp.bfloat16)


def body(tokens, gate_weights, expert_ids, w_gate, w_up, w_down):
    tok_count = tokens.shape[0]
    columns = lax.axis_size("grp")
    slot_depth = 2 * tok_count * RGROUPS // (columns * w_gate.shape[0])
    dense = slot_depth * w_gate.shape[0] >= tok_count
    fits = columns % 4 == 0 and lax.axis_size("loc") == 2 and tok_count % 32 == 0
    chosen = dense_body if dense and fits else slot_body
    return chosen(tokens, gate_weights, expert_ids, w_gate, w_up, w_down)


def solution(mesh):
    placed = (
        P(("grp", "loc"), None),
        P(("grp", "loc"), None),
        P(("grp", "loc"), None),
        P("grp", None, "loc"),
        P("grp", None, "loc"),
        P("grp", None, "loc"),
    )
    return jax.shard_map(
        body, mesh=mesh, in_specs=placed, out_specs=P(("grp", "loc"), None), check_vma=False
    )
```
